32 devices in a mesh: dp: 16 (over z, x, core), tensor: 2 (over y).
Axes of the slice: x: 2, y: 2, z: 4, core: 2. Of those that a mesh axis runs over, the one named last changes fastest.
Arguments:
- hidden_in: bfloat16 [6144, 4096], P('dp'), may hold values from -6 to 6
- upstream: bfloat16 [6144, 4096], P('dp'), may hold values from -6 to 6
- merged_input_weight: bfloat16 [4096, 6144], P('dp', 'tensor'), may hold values from -0.09375 to 0.09375
- output_matrix: bfloat16 [4096, 4096], P('dp', 'tensor'), may hold values from -0.09375 to 0.09375
- norm_gain: float32 [4096], replicated, may hold values from 0.5 to 1.5
- query_gain: float32 [128], replicated, may hold values from 0.5 to 1.5
- key_gain: float32 [128], replicated, may hold values from 0.5 to 1.5
Outputs:
- hidden_grad: bfloat16 [6144, 4096], P('dp')
- input_grad: float32 [4096, 6144], P('dp', 'tensor')
- output_grad: float32 [4096, 4096], P('dp', 'tensor')
- gain_grad: float32 [4096], replicated
- query_grad: float32 [128], replicated
- key_grad: float32 [128], replicated
The draws below stay inside these ranges and needn't reach their ends.
All inputs are finite; a program needn't handle non-finite values.
Results may differ from the reference program's by a relative error of at most 0.015.
Values may be sent and summed in bfloat16 or wider, within the bound.
A program may use at most 128 MiB of HBM per device.

```python
import math
from functools import partial
import jax
import jax.numpy as jnp
from jax import lax

MODEL_WIDTH = 4096
QUERY_HEADS = 32
KEY_VALUE_HEADS = 8
HEAD_SIZE = 128
SEQUENCE_LENGTH = 384
TOKENS = 6144
N_DP = 16
N_TENSOR = 2


def spiked(values, stream_key, source, target, shards_of, factor):
    def block_of(position):
        return (jnp.arange(values.shape[position]) // (values.shape[position] // shards_of)).reshape((-1,) + (1,) * (values.ndim - 1 - position))

    one_side = jax.random.permutation(stream_key, shards_of)[block_of(target)]
    second = (block_of(target) + shards_of // 2) % shards_of
    return jnp.where((block_of(source) == one_side) | (block_of(source) == second), factor * values, values)


def steps_of(key, dims, shards, least, largest):
    gain = 1.0
    for axis_at, shards_of in shards:
        steps = jax.random.uniform(jax.random.fold_in(jax.random.fold_in(key, 6), axis_at), (shards_of,), jnp.float32, least / len(shards), largest / len(shards))
        gain = gain * jnp.repeat(jnp.exp(steps), dims[axis_at] // shards_of).reshape((-1,) + (1,) * (len(dims) - 1 - axis_at))
    return gain


def gaussian(own_key, dims, spread, bound, shards=(), kind=jnp.bfloat16):
    array = jax.random.normal(own_key, dims, jnp.float32) * spread
    if len(shards) > 0:
        array = steps_of(own_key, dims, shards, -0.22, 0.18) * array
    return jnp.clip(array, min=-bound, max=bound).astype(kind)


def noise_with(stream_key, dims, scale, bound, split, heavy, held_as=jnp.bfloat16):
    drawn = scale * jax.random.normal(stream_key, dims, jnp.float32)
    if split:
        drawn = drawn * steps_of(stream_key, dims, split, -0.22, 0.18)
    return jnp.clip(spiked(drawn, jax.random.fold_in(stream_key, 3), *heavy), -bound, bound).astype(held_as)


def setup_inputs(seed: int = 0) -> dict:
    arg_keys = jax.random.split(jax.random.key(seed), 8)
    hidden_in = noise_with(arg_keys[0], (TOKENS, MODEL_WIDTH), 1.0, 6.0, ((0, 16),), (0, 1, 16, 2.0))
    upstream = noise_with(arg_keys[1], (TOKENS, MODEL_WIDTH), 1.0, 6.0, ((0, 16),), (0, 1, 16, 2.0))
    merged_input_weight = gaussian(arg_keys[2], (MODEL_WIDTH, (QUERY_HEADS + 2 * KEY_VALUE_HEADS) * HEAD_SIZE), MODEL_WIDTH ** -0.5, 0.09375, ((0, 16), (1, 2)))
    output_matrix = gaussian(arg_keys[3], (MODEL_WIDTH, QUERY_HEADS * HEAD_SIZE), (QUERY_HEADS * HEAD_SIZE) ** -0.5, 0.09375, ((0, 16), (1, 2)))
    norm_gain = jnp.clip(1.0 + 0.1 * jax.random.normal(arg_keys[4], (MODEL_WIDTH,), jnp.float32), 0.5, 1.5)
    query_gain = jnp.clip(1.0 + 0.1 * jax.random.normal(arg_keys[5], (HEAD_SIZE,), jnp.float32), 0.5, 1.5)
    key_gain = jnp.clip(1.0 + 0.1 * jax.random.normal(arg_keys[6], (HEAD_SIZE,), jnp.float32), 0.5, 1.5)
    return {"hidden_in": hidden_in, "upstream": upstream, "merged_input_weight": merged_input_weight, "output_matrix": output_matrix, "norm_gain": norm_gain, "query_gain": query_gain, "key_gain": key_gain}


EPSILON = 1e-06
ROPE_BASE = 1000000.0

def lowered_precision(value_rows):
    return lax.optimization_barrier(value_rows.astype(jnp.bfloat16))

def norm_rows(states, scaling):
    widened = states.astype(jnp.float32)
    inverse = lax.rsqrt(lax.optimization_barrier(jnp.mean(widened * widened, axis=-1, keepdims=True)) + EPSILON)
    return widened * inverse * scaling

def rope_tables(length, columns):
    half_width = columns // 2
    exponent = jnp.arange(half_width, dtype=jnp.float32) * (2.0 / columns)
    frequency = jnp.exp(-exponent * math.log(ROPE_BASE))
    places = jnp.arange(length, dtype=jnp.float32)
    angles = places[:, None] * frequency[None, :]
    return (jnp.cos(angles), jnp.sin(angles))

def head_post(projected_rows, scaling, cosine, sine):
    inverse = lax.rsqrt(lax.optimization_barrier(jnp.mean(projected_rows * projected_rows, axis=-1, keepdims=True)) + EPSILON)
    normed = projected_rows * inverse * scaling
    half_width = projected_rows.shape[-1] // 2
    layout = (projected_rows.shape[0],) + (1,) * (projected_rows.ndim - 2) + (half_width,)
    cosine_part = cosine.reshape(layout)
    sine_part = sine.reshape(layout)
    leading = normed[..., :half_width]
    trailing = normed[..., half_width:]
    return jnp.concatenate([leading * cosine_part - trailing * sine_part, trailing * cosine_part + leading * sine_part], axis=-1)

def widen(value_rows):
    return value_rows.astype(jnp.float32)

def reference(hidden_in, upstream, merged_input_weight, output_matrix, norm_gain, query_gain, key_gain):
    shard_ranks = N_TENSOR
    query_heads = QUERY_HEADS // shard_ranks
    key_head_rows = KEY_VALUE_HEADS // shard_ranks
    group_width = QUERY_HEADS // KEY_VALUE_HEADS
    attention_block = (QUERY_HEADS + 2 * KEY_VALUE_HEADS) * HEAD_SIZE // shard_ranks
    query_columns = query_heads * HEAD_SIZE
    key_columns = key_head_rows * HEAD_SIZE
    grad_scale = 1.0 / math.sqrt(TOKENS)
    score_scale = 1.0 / math.sqrt(HEAD_SIZE)
    cosine, sine = rope_tables(SEQUENCE_LENGTH, HEAD_SIZE)
    post = partial(head_post, cosine=cosine, sine=sine)
    weight_blocks = merged_input_weight.astype(jnp.float32).reshape(MODEL_WIDTH, shard_ranks, attention_block)
    causal = lax.broadcasted_iota(jnp.int32, (SEQUENCE_LENGTH, SEQUENCE_LENGTH), 0) >= lax.broadcasted_iota(jnp.int32, (SEQUENCE_LENGTH, SEQUENCE_LENGTH), 1)

    def one_sequence(carry, inputs):
        input_acc, output_acc, gain_acc, query_acc, key_acc = carry
        hidden, incoming_gradient = inputs
        local_norm, norm_back = jax.vjp(norm_rows, hidden.astype(jnp.float32), norm_gain)
        normed = lowered_precision(local_norm)
        projected_rows = jnp.dot(normed, merged_input_weight, preferred_element_type=jnp.float32).reshape(SEQUENCE_LENGTH, shard_ranks, attention_block)
        unnormed_query = projected_rows[:, :, :query_columns].reshape(SEQUENCE_LENGTH, KEY_VALUE_HEADS, group_width, HEAD_SIZE)
        unnormed_key = projected_rows[:, :, query_columns:query_columns + key_columns].reshape(SEQUENCE_LENGTH, KEY_VALUE_HEADS, HEAD_SIZE)
        value_rows = lowered_precision(projected_rows[:, :, query_columns + key_columns:].reshape(SEQUENCE_LENGTH, KEY_VALUE_HEADS, HEAD_SIZE))
        queries_full, query_back = jax.vjp(post, unnormed_query, query_gain)
        keys_full, key_back = jax.vjp(post, unnormed_key, key_gain)
        queries = lowered_precision(queries_full)
        keys = lowered_precision(keys_full)
        scores = jnp.einsum('tkgh,skh->kgts', widen(queries), widen(keys)) * score_scale
        raised = jnp.where(causal, jnp.exp(scores), 0.0)
        softmax = raised / lax.optimization_barrier(jnp.sum(raised, axis=-1, keepdims=True))
        softmax_low = lowered_precision(softmax)
        context = jnp.einsum('kgts,skh->tkgh', widen(softmax_low), widen(value_rows))
        context_low = lowered_precision(context).reshape(SEQUENCE_LENGTH, QUERY_HEADS * HEAD_SIZE)
        context_gradient = lowered_precision(jnp.dot(incoming_gradient, output_matrix, preferred_element_type=jnp.float32)).reshape(SEQUENCE_LENGTH, KEY_VALUE_HEADS, group_width, HEAD_SIZE)
        grad_probs = jnp.einsum('tkgh,skh->kgts', widen(context_gradient), widen(value_rows))
        centre = lax.optimization_barrier(jnp.sum(softmax * grad_probs, axis=-1, keepdims=True))
        grad_scores = lowered_precision(softmax * (grad_probs - centre) * score_scale)
        grad_values = jnp.einsum('kgts,tkgh->skh', widen(softmax_low), widen(context_gradient))
        grad_queries = jnp.einsum('kgts,skh->tkgh', widen(grad_scores), widen(keys))
        grad_keys = jnp.einsum('kgts,tkgh->skh', widen(grad_scores), widen(queries))
        grad_raw_query, query_part = query_back(grad_queries)
        grad_raw_key, key_part = key_back(grad_keys)
        grad_projected = lowered_precision(jnp.concatenate([grad_raw_query.reshape(SEQUENCE_LENGTH, shard_ranks, query_columns), grad_raw_key.reshape(SEQUENCE_LENGTH, shard_ranks, key_columns), grad_values.reshape(SEQUENCE_LENGTH, shard_ranks, key_columns)], axis=2).reshape(SEQUENCE_LENGTH, shard_ranks * attention_block))
        input_term = lowered_precision(jnp.dot(normed.T, grad_projected, preferred_element_type=jnp.float32) * grad_scale)
        output_term = lowered_precision(jnp.dot(incoming_gradient.T, context_low, preferred_element_type=jnp.float32) * grad_scale)
        rank_terms = jnp.einsum('trc,drc->rtd', widen(grad_projected).reshape(SEQUENCE_LENGTH, shard_ranks, attention_block), weight_blocks)
        grad_normed = lax.optimization_barrier(jnp.sum(widen(lowered_precision(rank_terms)), axis=0))
        grad_hidden, gain_part = norm_back(grad_normed)
        hidden_grad = (incoming_gradient.astype(jnp.float32) + grad_hidden).astype(jnp.bfloat16)
        carry = (input_acc + widen(input_term), output_acc + widen(output_term), gain_acc + gain_part, query_acc + query_part, key_acc + key_part)
        return (carry, hidden_grad)
    start_offset = (jnp.zeros((MODEL_WIDTH, (QUERY_HEADS + 2 * KEY_VALUE_HEADS) * HEAD_SIZE), jnp.float32), jnp.zeros((MODEL_WIDTH, QUERY_HEADS * HEAD_SIZE), jnp.float32), jnp.zeros((MODEL_WIDTH,), jnp.float32), jnp.zeros((HEAD_SIZE,), jnp.float32), jnp.zeros((HEAD_SIZE,), jnp.float32))
    sequences = (hidden_in.reshape(N_DP, SEQUENCE_LENGTH, MODEL_WIDTH), upstream.reshape(N_DP, SEQUENCE_LENGTH, MODEL_WIDTH))
    totals, hidden_parts = lax.scan(one_sequence, start_offset, sequences)
    input_grad, output_grad, gain_sum, query_sum, key_sum = totals
    return (hidden_parts.reshape(TOKENS, MODEL_WIDTH), input_grad, output_grad, gain_sum * grad_scale, query_sum * grad_scale, key_sum * grad_scale)
```

```python
from functools import partial
import math

import jax
import jax.numpy as jnp
from jax import lax
from jax.sharding import PartitionSpec as P

QUERY_HEADS = 32
KEY_VALUE_HEADS = 8
HEAD_SIZE = 128


EPSILON = 1e-06
ROPE_BASE = 1000000.0


def norm_rows(states, scaling):
    inverse = lax.rsqrt(jnp.mean(states * states, axis=-1, keepdims=True) + EPSILON)
    return states * inverse * scaling


def rope_tables(length, columns):
    half_width = columns // 2
    exponent = jnp.arange(half_width, dtype=jnp.float32) * (2.0 / columns)
    frequency = jnp.exp(-exponent * math.log(ROPE_BASE))
    places = jnp.arange(length, dtype=jnp.float32)
    angles = places[:, None] * frequency[None, :]
    return (jnp.cos(angles), jnp.sin(angles))


def head_post(projected_rows, scaling, cosine, sine):
    inverse = lax.rsqrt(jnp.mean(projected_rows * projected_rows, axis=-1, keepdims=True) + EPSILON)
    normed = projected_rows * inverse * scaling
    half_width = projected_rows.shape[-1] // 2
    layout = (projected_rows.shape[0],) + (1,) * (projected_rows.ndim - 2) + (half_width,)
    cosine_part = cosine.reshape(layout)
    sine_part = sine.reshape(layout)
    leading = normed[..., :half_width]
    trailing = normed[..., half_width:]
    return jnp.concatenate(
        [
            leading * cosine_part - trailing * sine_part,
            trailing * cosine_part + leading * sine_part,
        ],
        axis=-1,
    )


def attend_forward(queries, keys, value_rows, score_scale):
    length = queries.shape[0]
    scores = (
        jnp.einsum("tkgh,skh->kgts", queries, keys, preferred_element_type=jnp.float32)
        * score_scale
    )
    causal = lax.broadcasted_iota(jnp.int32, (length, length), 0) >= lax.broadcasted_iota(
        jnp.int32, (length, length), 1
    )
    raised = jnp.where(causal, jnp.exp(scores), 0.0)
    softmax = raised / jnp.sum(raised, axis=-1, keepdims=True)
    softmax_low = softmax.astype(jnp.bfloat16)
    context = jnp.einsum(
        "kgts,skh->tkgh", softmax_low, value_rows, preferred_element_type=jnp.float32
    )
    return (softmax, softmax_low, context)


def attend_backward(queries, keys, value_rows, softmax, softmax_low, context_gradient, score_scale):
    grad_probs = jnp.einsum(
        "tkgh,skh->kgts", context_gradient, value_rows, preferred_element_type=jnp.float32
    )
    centre = jnp.sum(softmax * grad_probs, axis=-1, keepdims=True)
    grad_scores = (softmax * (grad_probs - centre) * score_scale).astype(jnp.bfloat16)
    grad_values = jnp.einsum(
        "kgts,tkgh->skh", softmax_low, context_gradient, preferred_element_type=jnp.float32
    )
    grad_queries = jnp.einsum(
        "kgts,skh->tkgh", grad_scores, keys, preferred_element_type=jnp.float32
    )
    grad_keys = jnp.einsum(
        "kgts,tkgh->skh", grad_scores, queries, preferred_element_type=jnp.float32
    )
    return (grad_queries, grad_keys, grad_values)


def core_pairs(count):
    return [(i, i ^ 1) for i in range(count)]


def chip_ring(chips):
    return list(range(0, chips, 2)) + list(reversed(range(1, chips, 2)))


def ring_reduce_rows(left, right, order, forward):
    chips = len(order)
    rows = left.shape[1] // chips
    chip = lax.axis_index("dp") // 2
    place_of = [0] * chips
    for place, member in enumerate(order):
        place_of[member] = place
    place = jnp.asarray(place_of, jnp.int32)[chip]
    table = jnp.asarray(order, jnp.int32)
    sign = 1 if forward else -1
    pairs = []
    for at, member in enumerate(order):
        target = order[(at + sign) % chips]
        pairs += [(2 * member + core, 2 * target + core) for core in range(2)]

    def term(step):
        block = table[lax.rem(place + sign * (-1 - step) + 2 * chips, chips)]
        part = lax.dynamic_slice_in_dim(left, block * rows, rows, 1)
        return lax.dot_general(
            part, right, (((0,), (0,)), ((), ())), preferred_element_type=jnp.float32
        )

    total = term(0)
    for step in range(1, chips):
        total = lax.ppermute(total.astype(jnp.bfloat16), "dp", pairs).astype(jnp.float32) + term(step)
    return total


def weight_gradient(rows, rows_other, right, splits):
    groups = lax.axis_size("dp")
    order = chip_ring(groups // 2)
    core = lax.axis_index("dp") % 2
    half = right.shape[1] // 2
    kept = lax.dynamic_slice_in_dim(right, core * half, half, 1)
    sent = lax.dynamic_slice_in_dim(right, (1 - core) * half, half, 1)
    right_pair = jnp.concatenate([kept, lax.ppermute(sent, "dp", core_pairs(groups))], axis=0)
    left_pair = jnp.concatenate([rows, rows_other], axis=0)
    width = half // (2 * splits)
    pieces = [
        ring_reduce_rows(left_pair, right_pair[:, i * width : (i + 1) * width], order, i % 2 == 0)
        for i in range(2 * splits)
    ]
    summed = jnp.concatenate(pieces, axis=1)
    block = summed.shape[0] // 2
    own = lax.dynamic_slice_in_dim(summed, core * block, block, 0)
    other = lax.dynamic_slice_in_dim(summed, (1 - core) * block, block, 0)
    received = lax.ppermute(other, "dp", core_pairs(groups))
    first = core == 0
    return jnp.concatenate(
        [jnp.where(first, own, received), jnp.where(first, received, own)], axis=1
    )


def sum_all(values, axis):
    count = lax.axis_size(axis)
    if count & (count - 1):
        return lax.psum(values, axis)
    step = 1
    while step < count:
        values = values + lax.ppermute(values, axis, [(i, i ^ step) for i in range(count)])
        step *= 2
    return values


def local(hidden_in, upstream, merged_input_weight, output_matrix, norm_gain, query_gain, key_gain):
    shard_ranks = lax.axis_size("tensor")
    groups = lax.axis_size("dp")
    query_heads = QUERY_HEADS // shard_ranks
    key_head_rows = KEY_VALUE_HEADS // shard_ranks
    group_width = QUERY_HEADS // KEY_VALUE_HEADS
    query_columns = query_heads * HEAD_SIZE
    key_columns = key_head_rows * HEAD_SIZE
    score_scale = 1.0 / math.sqrt(HEAD_SIZE)
    length = hidden_in.shape[0]
    grad_scale = 1.0 / math.sqrt(groups * length)
    local_norm, norm_back = jax.vjp(norm_rows, hidden_in.astype(jnp.float32), norm_gain)
    normed = local_norm.astype(jnp.bfloat16)
    normed_other = lax.ppermute(normed, "dp", core_pairs(groups))
    upstream_other = lax.ppermute(upstream, "dp", core_pairs(groups))
    full_weight = lax.all_gather(merged_input_weight, "dp", axis=0, tiled=True)
    full_weight, output_matrix = lax.optimization_barrier((full_weight, output_matrix))
    projected_rows = jnp.dot(normed, full_weight, preferred_element_type=jnp.float32)
    unnormed_query = projected_rows[:, :query_columns].reshape(
        length, key_head_rows, group_width, HEAD_SIZE
    )
    unnormed_key = projected_rows[:, query_columns : query_columns + key_columns].reshape(
        length, key_head_rows, HEAD_SIZE
    )
    value_rows = (
        projected_rows[:, query_columns + key_columns :]
        .astype(jnp.bfloat16)
        .reshape(length, key_head_rows, HEAD_SIZE)
    )
    cosine, sine = rope_tables(length, HEAD_SIZE)
    post = partial(head_post, cosine=cosine, sine=sine)
    queries_full, query_back = jax.vjp(post, unnormed_query, query_gain)
    keys_full, key_back = jax.vjp(post, unnormed_key, key_gain)
    queries = queries_full.astype(jnp.bfloat16)
    keys = keys_full.astype(jnp.bfloat16)
    context_gradient = jnp.dot(
        upstream,
        lax.all_gather(output_matrix, "dp", axis=0, tiled=True),
        preferred_element_type=jnp.float32,
    )
    context_gradient = context_gradient.astype(jnp.bfloat16).reshape(
        length, key_head_rows, group_width, HEAD_SIZE
    )
    softmax, softmax_low, context = attend_forward(queries, keys, value_rows, score_scale)
    context_low = context.astype(jnp.bfloat16).reshape(length, query_columns)
    output_grad = weight_gradient(upstream, upstream_other, context_low, 1) * grad_scale
    grad_queries, grad_keys, grad_values = attend_backward(
        queries, keys, value_rows, softmax, softmax_low, context_gradient, score_scale
    )
    grad_raw_query, query_part = query_back(grad_queries)
    grad_raw_key, key_part = key_back(grad_keys)
    grad_projected = jnp.concatenate(
        [
            grad_raw_query.reshape(length, query_columns),
            grad_raw_key.reshape(length, key_columns),
            grad_values.reshape(length, key_columns),
        ],
        axis=1,
    ).astype(jnp.bfloat16)
    input_grad = weight_gradient(normed, normed_other, grad_projected, 2) * grad_scale
    share_normed = lax.dot_general(
        grad_projected, full_weight, (((1,), (1,)), ((), ())), preferred_element_type=jnp.float32
    ).astype(jnp.bfloat16)
    grad_normed = share_normed.astype(jnp.float32)
    for shift in range(1, shard_ranks):
        grad_normed = grad_normed + lax.ppermute(
            share_normed, "tensor", [(i, (i + shift) % shard_ranks) for i in range(shard_ranks)]
        ).astype(jnp.float32)
    grad_hidden, gain_part = norm_back(grad_normed)
    hidden_grad = (upstream.astype(jnp.float32) + grad_hidden).astype(jnp.bfloat16)
    gains = jnp.concatenate([gain_part * (1.0 / shard_ranks), query_part, key_part])
    gains = sum_all(sum_all(gains, "tensor"), "dp")
    width = gain_part.shape[0]
    gain_sum, query_sum, key_sum = jnp.split(gains, [width, width + HEAD_SIZE])
    return (
        hidden_grad,
        input_grad,
        output_grad,
        gain_sum * grad_scale,
        query_sum * grad_scale,
        key_sum * grad_scale,
    )


def solution(mesh):
    in_specs = (P("dp", None), P("dp", None), P("dp", "tensor"), P("dp", "tensor"), P(), P(), P())
    out_specs = (P("dp", None), P("dp", "tensor"), P("dp", "tensor"), P(), P(), P())
    return jax.shard_map(local, mesh=mesh, in_specs=in_specs, out_specs=out_specs, check_vma=False)
```
